512 devices in a mesh: blk: 512 (over x, y, z, core).
Axes of the slice: x: 4, y: 8, z: 8, core: 2. Of those that a mesh axis runs over, the one named last changes fastest.
Arguments:
- samples: bfloat16 [131072, 2048], P('blk'), may hold values from -6 to 6
- hubs: int32 [64], replicated, may hold values from 0 to 131071, as said below
- start: int32 [1], replicated, may hold values from 1 to 253
Outputs:
- self_stat: float32 [131072, 256], P('blk')
- ahead_stat: float32 [3, 131072, 256], P(None, 'blk')
- behind_stat: float32 [3, 131072, 256], P(None, 'blk')
The draws below stay inside these ranges and needn't reach their ends.
Inputs may be any that keep to these rules, and one draw needn't show every extreme that they name: `hubs`: the 64 indices are distinct.
All inputs are finite; a program needn't handle non-finite values.
Results may differ from the reference program's by a relative error of at most 0.0049.
Values may be sent and summed in bfloat16 or wider, within the bound.
A program may use at most 64 MiB of HBM per device.

```python
import math
import jax
import jax.numpy as jnp
from jax import lax

BLK = 256
SAMPLES = 2048
HUBS = 64
WINDOW = 3
TRANSCRIPTS = 131072
N_BLK = 512


def draw_hubs(key, part):
    order = jax.random.permutation(jax.random.fold_in(key, 11), TRANSCRIPTS)
    return order[:HUBS].astype(jnp.int32)


def block_levels(key, extent, pieces, smallest, top_value):
    factor_of, own = 1.0, jax.random.fold_in(key, 6)
    for position, parts in pieces:
        draws = jnp.exp(jax.random.uniform(jax.random.fold_in(own, position), (parts,), jnp.float32, smallest / len(pieces), top_value / len(pieces)))
        factor_of = factor_of * jnp.repeat(draws, extent[position] // parts).reshape([-1 if axis == position else 1 for axis in range(len(extent))])
    return factor_of


def noise(rng, shape, deviation, bound, pieces=(), kind=jnp.bfloat16):
    values = deviation * jax.random.normal(rng, shape, jnp.float32)
    if pieces:
        values = values * block_levels(rng, shape, pieces, -0.22, 0.18)
    return jnp.clip(values, -bound, bound).astype(kind)


def setup_inputs(seed: int = 0) -> dict:
    splits = jax.random.split(jax.random.key(seed), 4)
    return {
        "samples": noise(splits[0], (TRANSCRIPTS, SAMPLES), 1.0, 6.0, ((0, 512),)),
        "hubs": draw_hubs(jax.random.fold_in(splits[3], 71), 0),
        "start": jax.random.randint(splits[2], (1,), 1, N_BLK // 2 - 2).astype(jnp.int32),
    }


def fisher(values):
    return 0.5 * (jnp.log1p(values) - jnp.log1p(-values))

def reference(samples, hubs, start):
    hub_rows = samples[hubs].astype(jnp.float32)
    gram = jnp.dot(hub_rows, hub_rows.T, precision=lax.Precision.HIGHEST)
    proj = jnp.dot(samples.astype(jnp.float32), hub_rows.astype(jnp.bfloat16).T.astype(jnp.float32), preferred_element_type=jnp.float32)
    coef = jnp.linalg.solve(gram, proj.T).T
    resid = (samples.astype(jnp.float32) - jnp.dot(coef, hub_rows, precision=lax.Precision.HIGHEST)).astype(jnp.bfloat16)
    wide = resid.astype(jnp.float32)
    scale = 1.0 / jnp.sqrt(jnp.maximum(lax.optimization_barrier(jnp.sum(wide * wide, axis=1)), 1.0))
    blocks = wide.reshape(N_BLK, BLK, SAMPLES)
    scales = scale.reshape(N_BLK, BLK)
    factor = math.sqrt(SAMPLES - HUBS - 3)

    def corr_for(offset):
        other = jnp.roll(blocks, -offset, axis=0)
        other_scale = jnp.roll(scales, -offset, axis=0)
        dots = jnp.einsum('bis,bks->bik', blocks, other)
        return (dots * scales[:, :, None] * other_scale[:, None, :]).astype(jnp.bfloat16)

    def to_stat(rounded):
        return factor * fisher(lax.optimization_barrier(rounded).astype(jnp.float32))
    own = corr_for(jnp.int32(0))
    diag = jnp.eye(BLK, dtype=jnp.bool_)[None, :, :]
    own_stat = jnp.where(diag, 0.0, to_stat(own))
    ahead = []
    behind = []
    for j in range(WINDOW):
        offset = start[0] + j
        tiles = corr_for(offset)
        ahead.append(to_stat(tiles).reshape(TRANSCRIPTS, BLK))
        turned = jnp.transpose(jnp.roll(tiles, offset, axis=0), (0, 2, 1))
        behind.append(to_stat(turned).reshape(TRANSCRIPTS, BLK))
    return (own_stat.reshape(TRANSCRIPTS, BLK), jnp.stack(ahead), jnp.stack(behind))
```

```python
import functools
import math

import jax
import jax.numpy as jnp
from jax import lax
from jax.sharding import Mesh
from jax.sharding import PartitionSpec as P

BLK = ("blk_0", "blk_1", "blk_2", "blk_3")
NX, NY, NZ = 4, 8, 8
NDEV = 2 * NX * NY * NZ


def split_up(array, dim, peers):
    before, after = (array.shape[:dim], array.shape[dim + 1 :])
    return jnp.moveaxis(array.reshape(*before, peers, -1, *after), dim, 0)


def sent_and_summed(array, axis, dim):
    tiles = split_up(array, dim, lax.axis_size(axis))
    arrived = lax.all_to_all(tiles, axis, split_axis=0, concat_axis=0, tiled=True)
    return arrived.sum(axis=0)


def summed_rows(array, axes, dim):
    far, near = axes
    tiles = split_up(array, dim, lax.axis_size(far))
    nearer = sent_and_summed(tiles, near, dim + 1)
    arrived = lax.all_to_all(nearer, far, split_axis=0, concat_axis=0, tiled=True)
    return arrived.sum(axis=0)


def rows_for(lines, peers):
    spare = -lines.shape[0] % peers
    if not spare:
        return lines
    return jnp.concatenate([lines, jnp.zeros((spare, *lines.shape[1:]), lines.dtype)])


def sent_to_all(array, axis):
    copies = jnp.broadcast_to(array, (lax.axis_size(axis), *array.shape))
    return lax.all_to_all(copies, axis, split_axis=0, concat_axis=0, tiled=True)


def joined_along(tiles, dim):
    tiles = jnp.moveaxis(tiles, 0, dim)
    lengths = tiles.shape
    return tiles.reshape(*lengths[:dim], lengths[dim] * lengths[dim + 1], *lengths[dim + 2 :])


def gathered_by_axis(array, axes, dim):
    far, near = axes
    tiles = sent_to_all(sent_to_all(array, far), near)
    return joined_along(tiles.swapaxes(0, 1).reshape(-1, *array.shape), dim)


def nested_sum(array, axes):
    lines = array.reshape(-1)
    own = summed_rows(rows_for(lines, lax.axis_size(axes[0]) * lax.axis_size(axes[1])), axes, 0)
    whole = gathered_by_axis(own, axes, 0)
    return whole[: len(lines)].reshape(array.shape)


def moved_by(block, blocks):
    route = [((i - blocks) % NDEV, i) for i in range(NDEV)]
    return lax.ppermute(block, BLK, route) if blocks % NDEV else block


def signed_digit(value, base):
    digit = lax.rem(value + base // 2, base) - base // 2
    return digit, (value - digit) // base


def resid_of(block, hub_rows, inverse):
    exact = lax.Precision.HIGHEST
    proj = lax.dot_general(
        block, hub_rows, (((1,), (1,)), ((), ())), preferred_element_type=jnp.float32
    )
    half = jnp.dot(proj, inverse.T, precision=exact)
    coef = jnp.dot(half, inverse, precision=exact)
    fitted = jnp.dot(coef, hub_rows.astype(jnp.float32), precision=exact)
    return (block.astype(jnp.float32) - fitted).astype(jnp.bfloat16)


def row_scale(resid):
    wide = resid.astype(jnp.float32)
    return 1.0 / jnp.sqrt(jnp.maximum(jnp.sum(wide * wide, axis=1), 1.0))


def dots_of(rows, columns):
    return lax.dot_general(
        rows, columns, (((1,), (1,)), ((), ())), preferred_element_type=jnp.float32
    )


def to_stat(rounded, factor):
    values = lax.optimization_barrier(rounded).astype(jnp.float32)
    return factor * (0.5 * (jnp.log1p(values) - jnp.log1p(-values)))


def shards(samples, hubs, start):
    rows = samples.shape[0]
    width = samples.shape[1]
    factor = math.sqrt(width - hubs.shape[0] - 3)
    mine = lax.axis_index(BLK)
    owner = hubs // rows
    within = hubs % rows
    picker = jnp.logical_and(
        (owner == mine)[:, None], within[:, None] == jnp.arange(rows, dtype=jnp.int32)[None, :]
    ).astype(jnp.bfloat16)
    picked = jnp.dot(picker, samples, preferred_element_type=jnp.float32).astype(jnp.bfloat16)

    chips = (start[0] + 1) // 2
    back = start[0] % 2
    dz, rest = signed_digit(chips, NZ)
    dy, dx = signed_digit(rest, NY)

    def first(step, samples, picked):
        up, dn = moved_by(samples, 2 * step), moved_by(samples, -2 * step)
        near = [moved_by(samples, t) for t in (2, 1, -1, -2)]
        hub_rows = nested_sum(picked, (("blk_0", "blk_1"), ("blk_2", "blk_3")))
        return up, dn, *near, hub_rows

    def second(step, up, dn, own, lo2, lo1, hi1, hi2, hub_rows):
        stride = 2 * NZ * step
        up, dn = moved_by(up, stride), moved_by(dn, -stride)
        wide = hub_rows.astype(jnp.float32)
        gram = jnp.dot(wide, wide.T, precision=lax.Precision.HIGHEST)
        lower = jnp.linalg.cholesky(gram)
        eye = jnp.eye(gram.shape[0], dtype=jnp.float32)
        inverse = jax.scipy.linalg.solve_triangular(lower, eye, lower=True)
        resids = [resid_of(block, hub_rows, inverse) for block in (own, lo2, lo1, hi1, hi2)]
        return up, dn, *resids, inverse

    def third(step, up, dn):
        stride = 2 * NZ * NY * step
        return moved_by(up, stride), moved_by(dn, -stride)

    firsts = [functools.partial(first, step) for step in range(-4, 4)]
    seconds = [functools.partial(second, step) for step in range(-4, 4)]
    thirds = [functools.partial(third, step) for step in range(3)]
    up, dn, lo2, lo1, hi1, hi2, hub_rows = lax.switch(dz + 4, firsts, samples, picked)
    up, dn, resid, lo2, lo1, hi1, hi2, inverse = lax.switch(
        dy + 4, seconds, up, dn, samples, lo2, lo1, hi1, hi2, hub_rows
    )
    up, dn = lax.switch(dx, thirds, up, dn)
    up, dn = resid_of(up, hub_rows, inverse), resid_of(dn, hub_rows, inverse)

    scales = {0: row_scale(resid), 1: row_scale(hi1), 2: row_scale(hi2)}
    scales.update({-1: row_scale(lo1), -2: row_scale(lo2)})
    blocks = {0: resid, 1: hi1, 2: hi2, -1: lo1, -2: lo2}
    own = dots_of(resid, resid) * scales[0][:, None] * scales[0][None, :]
    own = own.astype(jnp.bfloat16)
    diag = jnp.arange(rows)[:, None] == jnp.arange(rows)[None, :]
    own_stat = jnp.where(diag, 0.0, to_stat(own, factor))

    scale_up, scale_dn = row_scale(up), row_scale(dn)

    def ahead_tile(t):
        tile = dots_of(blocks[-t], dn) * scales[-t][:, None] * scale_dn[None, :]
        return tile.astype(jnp.bfloat16)

    def behind_tile(t):
        tile = dots_of(blocks[t], up) * scale_up[None, :] * scales[t][:, None]
        return tile.astype(jnp.bfloat16)

    odd = back == 1
    w = jnp.stack([ahead_tile(t) for t in range(-1, 3)])
    v = jnp.stack([behind_tile(t) for t in range(-1, 3)])
    w = jnp.where(odd, w[:3], w[1:])
    v = jnp.where(odd, v[:3], v[1:])

    def swapped(which, w, v):
        moves = [j - which for j in range(3)]
        a = [moved_by(w[j], -t) for j, t in enumerate(moves)]
        b = [moved_by(v[j], t) for j, t in enumerate(moves)]
        return jnp.stack(a), jnp.stack(b)

    a, b = lax.switch(back, [functools.partial(swapped, which) for which in range(2)], w, v)
    return (own_stat, to_stat(a, factor), to_stat(b, factor))


def solution(mesh):
    split = Mesh(mesh.devices.reshape(NX, NY, NZ, 2), BLK)
    placed = (P(BLK, None), P(), P())
    return jax.shard_map(
        shards,
        mesh=split,
        in_specs=placed,
        out_specs=(P(BLK, None), P(None, BLK, None), P(None, BLK, None)),
        check_vma=False,
    )
```

```python
import functools
import math

import jax
import jax.numpy as jnp
from jax import lax
from jax.sharding import Mesh
from jax.sharding import PartitionSpec as P

BLK = ("blk_0", "blk_1", "blk_2", "blk_3")
NX, NY, NZ = 4, 8, 8
NDEV = 2 * NX * NY * NZ


def split_up(array, dim, peers):
    before, after = (array.shape[:dim], array.shape[dim + 1 :])
    return jnp.moveaxis(array.reshape(*before, peers, -1, *after), dim, 0)


def sent_and_summed(array, axis, dim):
    tiles = split_up(array, dim, lax.axis_size(axis))
    arrived = lax.all_to_all(tiles, axis, split_axis=0, concat_axis=0, tiled=True)
    return arrived.sum(axis=0)


def summed_rows(array, axes, dim):
    far, near = axes
    tiles = split_up(array, dim, lax.axis_size(far))
    nearer = sent_and_summed(tiles, near, dim + 1)
    arrived = lax.all_to_all(nearer, far, split_axis=0, concat_axis=0, tiled=True)
    return arrived.sum(axis=0)


def rows_for(lines, peers):
    spare = -lines.shape[0] % peers
    if not spare:
        return lines
    return jnp.concatenate([lines, jnp.zeros((spare, *lines.shape[1:]), lines.dtype)])


def sent_to_all(array, axis):
    copies = jnp.broadcast_to(array, (lax.axis_size(axis), *array.shape))
    return lax.all_to_all(copies, axis, split_axis=0, concat_axis=0, tiled=True)


def joined_along(tiles, dim):
    tiles = jnp.moveaxis(tiles, 0, dim)
    lengths = tiles.shape
    return tiles.reshape(*lengths[:dim], lengths[dim] * lengths[dim + 1], *lengths[dim + 2 :])


def gathered_by_axis(array, axes, dim):
    far, near = axes
    tiles = sent_to_all(sent_to_all(array, far), near)
    return joined_along(tiles.swapaxes(0, 1).reshape(-1, *array.shape), dim)


def nested_sum(array, axes):
    lines = array.reshape(-1)
    own = summed_rows(rows_for(lines, lax.axis_size(axes[0]) * lax.axis_size(axes[1])), axes, 0)
    whole = gathered_by_axis(own, axes, 0)
    return whole[: len(lines)].reshape(array.shape)


def moved_by(block, blocks):
    route = [((i - blocks) % NDEV, i) for i in range(NDEV)]
    return lax.ppermute(block, BLK, route) if blocks % NDEV else block


def signed_digit(value, base):
    digit = lax.rem(value + base // 2, base) - base // 2
    return digit, (value - digit) // base


def resid_of(block, hub_rows, inverse):
    exact = lax.Precision.HIGHEST
    proj = lax.dot_general(
        block, hub_rows, (((1,), (1,)), ((), ())), preferred_element_type=jnp.float32
    )
    half = jnp.dot(proj, inverse.T, precision=exact)
    coef = jnp.dot(half, inverse, precision=exact)
    fitted = jnp.dot(coef, hub_rows.astype(jnp.float32), precision=exact)
    return (block.astype(jnp.float32) - fitted).astype(jnp.bfloat16)


def row_scale(resid):
    wide = resid.astype(jnp.float32)
    return 1.0 / jnp.sqrt(jnp.maximum(jnp.sum(wide * wide, axis=1), 1.0))


def dots_of(rows, columns):
    return lax.dot_general(
        rows, columns, (((1,), (1,)), ((), ())), preferred_element_type=jnp.float32
    )


def to_stat(rounded, factor):
    values = lax.optimization_barrier(rounded).astype(jnp.float32)
    return factor * (0.5 * (jnp.log1p(values) - jnp.log1p(-values)))


def shards(samples, hubs, start):
    rows = samples.shape[0]
    width = samples.shape[1]
    factor = math.sqrt(width - hubs.shape[0] - 3)
    mine = lax.axis_index(BLK)
    owner = hubs // rows
    within = hubs % rows
    picker = jnp.logical_and(
        (owner == mine)[:, None], within[:, None] == jnp.arange(rows, dtype=jnp.int32)[None, :]
    ).astype(jnp.bfloat16)
    picked = jnp.dot(picker, samples, preferred_element_type=jnp.float32).astype(jnp.bfloat16)

    chips = (start[0] + 1) // 2
    back = start[0] % 2
    dz, rest = signed_digit(chips, NZ)
    dy, dx = signed_digit(rest, NY)

    hub_rows = nested_sum(picked, (("blk_0", "blk_1"), ("blk_2", "blk_3")))

    def first(step, samples, hub_rows):
        stride = 2 * NZ * NY * step
        up, dn = moved_by(samples, stride), moved_by(samples, -stride)
        wide = hub_rows.astype(jnp.float32)
        gram = jnp.dot(wide, wide.T, precision=lax.Precision.HIGHEST)
        lower = jnp.linalg.cholesky(gram)
        eye = jnp.eye(gram.shape[0], dtype=jnp.float32)
        inverse = jax.scipy.linalg.solve_triangular(lower, eye, lower=True)
        return up, dn, resid_of(samples, hub_rows, inverse), inverse

    def further(stride, up, dn):
        return moved_by(up, stride), moved_by(dn, -stride)

    firsts = [functools.partial(first, step) for step in range(3)]
    seconds = [functools.partial(further, 2 * NZ * step) for step in range(-4, 4)]
    thirds = [functools.partial(further, 2 * step) for step in range(-4, 4)]
    up, dn, resid, inverse = lax.switch(dx, firsts, samples, hub_rows)
    lo2, lo1, hi1, hi2 = (moved_by(resid, t) for t in (2, 1, -1, -2))
    up, dn = lax.switch(dy + 4, seconds, up, dn)
    up, dn = lax.switch(dz + 4, thirds, up, dn)
    up, dn = resid_of(up, hub_rows, inverse), resid_of(dn, hub_rows, inverse)

    scales = {0: row_scale(resid), 1: row_scale(hi1), 2: row_scale(hi2)}
    scales.update({-1: row_scale(lo1), -2: row_scale(lo2)})
    blocks = {0: resid, 1: hi1, 2: hi2, -1: lo1, -2: lo2}
    own = dots_of(resid, resid) * scales[0][:, None] * scales[0][None, :]
    own = own.astype(jnp.bfloat16)
    diag = jnp.arange(rows)[:, None] == jnp.arange(rows)[None, :]
    own_stat = jnp.where(diag, 0.0, to_stat(own, factor))

    scale_up, scale_dn = row_scale(up), row_scale(dn)

    def ahead_tile(t):
        tile = dots_of(blocks[-t], dn) * scales[-t][:, None] * scale_dn[None, :]
        return tile.astype(jnp.bfloat16)

    def behind_tile(t):
        tile = dots_of(blocks[t], up) * scale_up[None, :] * scales[t][:, None]
        return tile.astype(jnp.bfloat16)

    odd = back == 1
    w = jnp.stack([ahead_tile(t) for t in range(-1, 3)])
    v = jnp.stack([behind_tile(t) for t in range(-1, 3)])
    w = jnp.where(odd, w[:3], w[1:])
    v = jnp.where(odd, v[:3], v[1:])

    def swapped(which, w, v):
        moves = [j - which for j in range(3)]
        a = [moved_by(w[j], -t) for j, t in enumerate(moves)]
        b = [moved_by(v[j], t) for j, t in enumerate(moves)]
        return jnp.stack(a), jnp.stack(b)

    a, b = lax.switch(back, [functools.partial(swapped, which) for which in range(2)], w, v)
    return (own_stat, to_stat(a, factor), to_stat(b, factor))


def solution(mesh):
    split = Mesh(mesh.devices.reshape(NX, NY, NZ, 2), BLK)
    placed = (P(BLK, None), P(), P())
    return jax.shard_map(
        shards,
        mesh=split,
        in_specs=placed,
        out_specs=(P(BLK, None), P(None, BLK, None), P(None, BLK, None)),
        check_vma=False,
    )
```

```python
import functools
import math

import jax
import jax.numpy as jnp
from jax import lax
from jax.experimental import pallas as pl
from jax.experimental.pallas import tpu as pltpu
from jax.sharding import Mesh
from jax.sharding import PartitionSpec as P

BLK = ("blk_0", "blk_1", "blk_2", "blk_3")
NX, NY, NZ = 4, 8, 8
NDEV = 2 * NX * NY * NZ


def split_up(array, dim, peers):
    before, after = (array.shape[:dim], array.shape[dim + 1 :])
    return jnp.moveaxis(array.reshape(*before, peers, -1, *after), dim, 0)


def sent_and_summed(array, axis, dim):
    tiles = split_up(array, dim, lax.axis_size(axis))
    arrived = lax.all_to_all(tiles, axis, split_axis=0, concat_axis=0, tiled=True)
    return arrived.sum(axis=0)


def summed_rows(array, axes, dim):
    far, near = axes
    tiles = split_up(array, dim, lax.axis_size(far))
    nearer = sent_and_summed(tiles, near, dim + 1)
    arrived = lax.all_to_all(nearer, far, split_axis=0, concat_axis=0, tiled=True)
    return arrived.sum(axis=0)


def rows_for(lines, peers):
    spare = -lines.shape[0] % peers
    if not spare:
        return lines
    return jnp.concatenate([lines, jnp.zeros((spare, *lines.shape[1:]), lines.dtype)])


def sent_to_all(array, axis):
    copies = jnp.broadcast_to(array, (lax.axis_size(axis), *array.shape))
    return lax.all_to_all(copies, axis, split_axis=0, concat_axis=0, tiled=True)


def joined_along(tiles, dim):
    tiles = jnp.moveaxis(tiles, 0, dim)
    lengths = tiles.shape
    return tiles.reshape(*lengths[:dim], lengths[dim] * lengths[dim + 1], *lengths[dim + 2 :])


def gathered_by_axis(array, axes, dim):
    far, near = axes
    tiles = sent_to_all(sent_to_all(array, far), near)
    return joined_along(tiles.swapaxes(0, 1).reshape(-1, *array.shape), dim)


def nested_sum(array, axes):
    lines = array.reshape(-1)
    own = summed_rows(rows_for(lines, lax.axis_size(axes[0]) * lax.axis_size(axes[1])), axes, 0)
    whole = gathered_by_axis(own, axes, 0)
    return whole[: len(lines)].reshape(array.shape)


def moved_by(block, blocks):
    route = [((i - blocks) % NDEV, i) for i in range(NDEV)]
    return lax.ppermute(block, BLK, route) if blocks % NDEV else block


def signed_digit(value, base):
    digit = lax.rem(value + base // 2, base) - base // 2
    return digit, (value - digit) // base


def resid_of(block, hub_rows, inverse):
    exact = lax.Precision.HIGHEST
    proj = lax.dot_general(
        block, hub_rows, (((1,), (1,)), ((), ())), preferred_element_type=jnp.float32
    )
    half = jnp.dot(proj, inverse.T, precision=exact)
    coef = jnp.dot(half, inverse, precision=exact)
    fitted = jnp.dot(coef, hub_rows.astype(jnp.float32), precision=exact)
    return (block.astype(jnp.float32) - fitted).astype(jnp.bfloat16)


def outer_dots(rows, columns):
    return lax.dot_general(
        rows, columns, (((1,), (1,)), ((), ())), preferred_element_type=jnp.float32
    )


def tiles_kernel(odd_ref, up_ref, dn_ref, own_ref, lo2, lo1, hi1, hi2, hub_ref, inv_ref, *outs):
    own_out, w_ref, v_ref, up_res, dn_res = outs
    odd = odd_ref[0] == 1
    exact = lax.Precision.HIGHEST
    hub, inverse = hub_ref[...], inv_ref[...]

    def residual(src, dst):
        block = src[...]
        proj = outer_dots(block, hub)
        half = lax.dot_general(
            proj, inverse, (((1,), (1,)), ((), ())),
            precision=exact, preferred_element_type=jnp.float32,
        )
        rest = jnp.dot(half, inverse, precision=exact, preferred_element_type=jnp.float32)
        pieces = []
        for _ in range(3):
            pieces.append(rest.astype(jnp.bfloat16))
            rest = rest - pieces[-1].astype(jnp.float32)
        for c in range(0, hub.shape[1], 512):
            columns = pl.ds(c, 512)
            part = hub_ref[:, columns]
            fitted = sum(
                jnp.dot(piece, part, preferred_element_type=jnp.float32) for piece in pieces[::-1]
            )
            dst[:, columns] = (src[:, columns].astype(jnp.float32) - fitted).astype(jnp.bfloat16)

    residual(up_ref, up_res)
    residual(dn_ref, dn_res)

    def scale(ref):
        wide = ref[...].astype(jnp.float32)
        return 1.0 / jnp.sqrt(jnp.maximum(jnp.sum(wide * wide, axis=1, keepdims=True), 1.0))

    def turned(column):
        return jnp.transpose(jnp.broadcast_to(column, (column.shape[0], 128)))[:1, :]

    refs = {0: own_ref, 1: hi1, 2: hi2, -1: lo1, -2: lo2}
    scales = {t: scale(ref) for t, ref in refs.items()}
    own = outer_dots(own_ref[...], own_ref[...]) * scales[0] * turned(scales[0])
    own_out[...] = own.astype(jnp.bfloat16)
    up_row, dn_row = turned(scale(up_res)), turned(scale(dn_res))
    for j in range(3):
        def chosen(sign):
            here, there = sign * (j - 1), sign * j
            block = jnp.where(odd, refs[here][...], refs[there][...])
            return block, jnp.where(odd, scales[here], scales[there])

        block, rows = chosen(-1)
        w_ref[j] = (outer_dots(block, dn_res[...]) * rows * dn_row).astype(jnp.bfloat16)
        block, rows = chosen(1)
        v_ref[j] = (outer_dots(block, up_res[...]) * up_row * rows).astype(jnp.bfloat16)


def tiles_of(odd, *arrays):
    rows, dtype = arrays[0].shape[0], arrays[0].dtype
    vmem = pl.BlockSpec(memory_space=pltpu.VMEM)
    return pl.pallas_call(
        tiles_kernel,
        out_shape=[
            jax.ShapeDtypeStruct((rows, rows), dtype),
            jax.ShapeDtypeStruct((3, rows, rows), dtype),
            jax.ShapeDtypeStruct((3, rows, rows), dtype),
        ],
        in_specs=[pl.BlockSpec(memory_space=pltpu.SMEM)] + [vmem] * len(arrays),
        out_specs=[vmem] * 3,
        scratch_shapes=[pltpu.VMEM(arrays[0].shape, dtype)] * 2,
        compiler_params=pltpu.CompilerParams(vmem_limit_bytes=48 * 1024 * 1024),
        cost_estimate=pl.CostEstimate(
            flops=14 * rows * rows * arrays[0].shape[1],
            bytes_accessed=8 * arrays[0].size,
            transcendentals=0,
        ),
        name="tiles",
    )(odd, *arrays)


def to_stat(rounded, factor):
    values = lax.optimization_barrier(rounded).astype(jnp.float32)
    return factor * (0.5 * (jnp.log1p(values) - jnp.log1p(-values)))


def shards(samples, hubs, start):
    rows = samples.shape[0]
    width = samples.shape[1]
    factor = math.sqrt(width - hubs.shape[0] - 3)
    mine = lax.axis_index(BLK)
    owner = hubs // rows
    within = hubs % rows
    picker = jnp.logical_and(
        (owner == mine)[:, None], within[:, None] == jnp.arange(rows, dtype=jnp.int32)[None, :]
    ).astype(jnp.bfloat16)
    picked = jnp.dot(picker, samples, preferred_element_type=jnp.float32).astype(jnp.bfloat16)

    chips = (start[0] + 1) // 2
    back = start[0] % 2
    dz, rest = signed_digit(chips, NZ)
    dy, dx = signed_digit(rest, NY)

    hub_rows = nested_sum(picked, (("blk_0", "blk_1"), ("blk_2", "blk_3")))

    def first(step, samples, hub_rows):
        stride = 2 * NZ * NY * step
        up, dn = moved_by(samples, stride), moved_by(samples, -stride)
        wide = hub_rows.astype(jnp.float32)
        gram = jnp.dot(wide, wide.T, precision=lax.Precision.HIGHEST)
        lower = jnp.linalg.cholesky(gram)
        eye = jnp.eye(gram.shape[0], dtype=jnp.float32)
        inverse = jax.scipy.linalg.solve_triangular(lower, eye, lower=True)
        return up, dn, resid_of(samples, hub_rows, inverse), inverse

    def further(stride, up, dn):
        return moved_by(up, stride), moved_by(dn, -stride)

    firsts = [functools.partial(first, step) for step in range(3)]
    seconds = [functools.partial(further, 2 * NZ * step) for step in range(-4, 4)]
    thirds = [functools.partial(further, 2 * step) for step in range(-4, 4)]
    up, dn, resid, inverse = lax.switch(dx, firsts, samples, hub_rows)
    lo2, lo1, hi1, hi2 = (moved_by(resid, t) for t in (2, 1, -1, -2))
    up, dn = lax.switch(dy + 4, seconds, up, dn)
    up, dn = lax.switch(dz + 4, thirds, up, dn)
    blocks = up, dn, resid, lo2, lo1, hi1, hi2
    own, w, v = tiles_of(start % 2, *blocks, hub_rows, inverse)
    diag = jnp.arange(rows)[:, None] == jnp.arange(rows)[None, :]
    own_stat = jnp.where(diag, 0.0, to_stat(own, factor))

    def swapped(which, w, v):
        moves = [j - which for j in range(3)]
        a = [moved_by(w[j], -t) for j, t in enumerate(moves)]
        b = [moved_by(v[j], t) for j, t in enumerate(moves)]
        return jnp.stack(a), jnp.stack(b)

    a, b = lax.switch(back, [functools.partial(swapped, which) for which in range(2)], w, v)
    return (own_stat, to_stat(a, factor), to_stat(b, factor))


def solution(mesh):
    split = Mesh(mesh.devices.reshape(NX, NY, NZ, 2), BLK)
    placed = (P(BLK, None), P(), P())
    return jax.shard_map(
        shards,
        mesh=split,
        in_specs=placed,
        out_specs=(P(BLK, None), P(None, BLK, None), P(None, BLK, None)),
        check_vma=False,
    )
```

```python
import functools
import math

import jax
import jax.numpy as jnp
from jax import lax
from jax.experimental import pallas as pl
from jax.experimental.pallas import tpu as pltpu
from jax.sharding import Mesh
from jax.sharding import PartitionSpec as P

BLK = ("blk_0", "blk_1", "blk_2", "blk_3")
NX, NY, NZ = 4, 8, 8
NDEV = 2 * NX * NY * NZ


def split_up(array, dim, peers):
    before, after = (array.shape[:dim], array.shape[dim + 1 :])
    return jnp.moveaxis(array.reshape(*before, peers, -1, *after), dim, 0)


def sent_and_summed(array, axis, dim):
    tiles = split_up(array, dim, lax.axis_size(axis))
    arrived = lax.all_to_all(tiles, axis, split_axis=0, concat_axis=0, tiled=True)
    return arrived.sum(axis=0)


def summed_rows(array, axes, dim):
    far, near = axes
    tiles = split_up(array, dim, lax.axis_size(far))
    nearer = sent_and_summed(tiles, near, dim + 1)
    arrived = lax.all_to_all(nearer, far, split_axis=0, concat_axis=0, tiled=True)
    return arrived.sum(axis=0)


def rows_for(lines, peers):
    spare = -lines.shape[0] % peers
    if not spare:
        return lines
    return jnp.concatenate([lines, jnp.zeros((spare, *lines.shape[1:]), lines.dtype)])


def sent_to_all(array, axis):
    copies = jnp.broadcast_to(array, (lax.axis_size(axis), *array.shape))
    return lax.all_to_all(copies, axis, split_axis=0, concat_axis=0, tiled=True)


def joined_along(tiles, dim):
    tiles = jnp.moveaxis(tiles, 0, dim)
    lengths = tiles.shape
    return tiles.reshape(*lengths[:dim], lengths[dim] * lengths[dim + 1], *lengths[dim + 2 :])


def gathered_by_axis(array, axes, dim):
    far, near = axes
    tiles = sent_to_all(sent_to_all(array, far), near)
    return joined_along(tiles.swapaxes(0, 1).reshape(-1, *array.shape), dim)


def nested_sum(array, axes):
    lines = array.reshape(-1)
    own = summed_rows(rows_for(lines, lax.axis_size(axes[0]) * lax.axis_size(axes[1])), axes, 0)
    whole = gathered_by_axis(own, axes, 0)
    return whole[: len(lines)].reshape(array.shape)


def moved_by(block, blocks):
    route = [((i - blocks) % NDEV, i) for i in range(NDEV)]
    return lax.ppermute(block, BLK, route) if blocks % NDEV else block


def signed_digit(value, base):
    digit = lax.rem(value + base // 2, base) - base // 2
    return digit, (value - digit) // base


def resid_of(block, hub_rows, inverse):
    exact = lax.Precision.HIGHEST
    proj = lax.dot_general(
        block, hub_rows, (((1,), (1,)), ((), ())), preferred_element_type=jnp.float32
    )
    half = jnp.dot(proj, inverse.T, precision=exact)
    coef = jnp.dot(half, inverse, precision=exact)
    fitted = jnp.dot(coef, hub_rows.astype(jnp.float32), precision=exact)
    return (block.astype(jnp.float32) - fitted).astype(jnp.bfloat16)


def outer_dots(rows, columns):
    return lax.dot_general(
        rows, columns, (((1,), (1,)), ((), ())), preferred_element_type=jnp.float32
    )


def tiles_kernel(odd_ref, up_ref, dn_ref, own_ref, lo2, lo1, hi1, hi2, hub_ref, inv_ref, *outs):
    own_out, w_ref, v_ref, up_res, dn_res = outs
    odd = odd_ref[0] == 1
    exact = lax.Precision.HIGHEST
    hub, inverse = hub_ref[...], inv_ref[...]

    def residual(src, dst):
        block = src[...]
        proj = outer_dots(block, hub)
        half = lax.dot_general(
            proj, inverse, (((1,), (1,)), ((), ())),
            precision=exact, preferred_element_type=jnp.float32,
        )
        rest = jnp.dot(half, inverse, precision=exact, preferred_element_type=jnp.float32)
        pieces = []
        for _ in range(3):
            pieces.append(rest.astype(jnp.bfloat16))
            rest = rest - pieces[-1].astype(jnp.float32)
        for c in range(0, hub.shape[1], 512):
            columns = pl.ds(c, 512)
            part = hub_ref[:, columns]
            fitted = sum(
                jnp.dot(piece, part, preferred_element_type=jnp.float32) for piece in pieces[::-1]
            )
            dst[:, columns] = (src[:, columns].astype(jnp.float32) - fitted).astype(jnp.bfloat16)

    residual(up_ref, up_res)
    residual(dn_ref, dn_res)

    def scale(ref):
        wide = ref[...].astype(jnp.float32)
        return 1.0 / jnp.sqrt(jnp.maximum(jnp.sum(wide * wide, axis=1, keepdims=True), 1.0))

    def turned(column):
        return jnp.transpose(jnp.broadcast_to(column, (column.shape[0], 128)))[:1, :]

    refs = {0: own_ref, 1: hi1, 2: hi2, -1: lo1, -2: lo2}
    scales = {t: scale(ref) for t, ref in refs.items()}
    own = outer_dots(own_ref[...], own_ref[...]) * scales[0] * turned(scales[0])
    own_out[...] = own.astype(jnp.bfloat16)
    up_row, dn_row = turned(scale(up_res)), turned(scale(dn_res))
    for j in range(3):
        def chosen(sign):
            here, there = sign * (j - 1), sign * j
            block = jnp.where(odd, refs[here][...], refs[there][...])
            return block, jnp.where(odd, scales[here], scales[there])

        block, rows = chosen(-1)
        w_ref[j] = (outer_dots(block, dn_res[...]) * rows * dn_row).astype(jnp.bfloat16)
        block, rows = chosen(1)
        v_ref[j] = (outer_dots(block, up_res[...]) * up_row * rows).astype(jnp.bfloat16)


def tiles_of(odd, *arrays):
    rows, dtype = arrays[0].shape[0], arrays[0].dtype
    vmem = pl.BlockSpec(memory_space=pltpu.VMEM)
    return pl.pallas_call(
        tiles_kernel,
        out_shape=[
            jax.ShapeDtypeStruct((rows, rows), dtype),
            jax.ShapeDtypeStruct((3, rows, rows), dtype),
            jax.ShapeDtypeStruct((3, rows, rows), dtype),
        ],
        in_specs=[pl.BlockSpec(memory_space=pltpu.SMEM)] + [vmem] * len(arrays),
        out_specs=[vmem] * 3,
        scratch_shapes=[pltpu.VMEM(arrays[0].shape, dtype)] * 2,
        compiler_params=pltpu.CompilerParams(vmem_limit_bytes=48 * 1024 * 1024),
        cost_estimate=pl.CostEstimate(
            flops=14 * rows * rows * arrays[0].shape[1],
            bytes_accessed=8 * arrays[0].size,
            transcendentals=0,
        ),
        name="tiles",
    )(odd, *arrays)


def to_stat(rounded, factor):
    values = lax.optimization_barrier(rounded).astype(jnp.float32)
    return factor * (0.5 * (jnp.log1p(values) - jnp.log1p(-values)))


def shards(samples, hubs, start):
    rows = samples.shape[0]
    width = samples.shape[1]
    factor = math.sqrt(width - hubs.shape[0] - 3)
    mine = lax.axis_index(BLK)
    owner = hubs // rows
    within = hubs % rows
    picker = jnp.logical_and(
        (owner == mine)[:, None], within[:, None] == jnp.arange(rows, dtype=jnp.int32)[None, :]
    ).astype(jnp.bfloat16)
    picked = jnp.dot(picker, samples, preferred_element_type=jnp.float32).astype(jnp.bfloat16)

    chips = (start[0] + 1) // 2
    back = start[0] % 2
    dz, rest = signed_digit(chips, NZ)
    dy, dx = signed_digit(rest, NY)

    def further(stride, up, dn):
        return moved_by(up, stride), moved_by(dn, -stride)

    def first(step, samples, picked):
        far = further(2 * NZ * NY * step, samples, samples)
        return *far, nested_sum(picked, (("blk_0", "blk_1"), ("blk_2", "blk_3")))

    def second(step, up, dn, samples, hub_rows):
        up, dn = further(2 * step, up, dn)
        wide = hub_rows.astype(jnp.float32)
        gram = jnp.dot(wide, wide.T, precision=lax.Precision.HIGHEST)
        lower = jnp.linalg.cholesky(gram)
        eye = jnp.eye(gram.shape[0], dtype=jnp.float32)
        inverse = jax.scipy.linalg.solve_triangular(lower, eye, lower=True)
        return up, dn, resid_of(samples, hub_rows, inverse), inverse

    firsts = [functools.partial(first, step) for step in range(3)]
    seconds = [functools.partial(second, step) for step in range(-4, 4)]
    thirds = [functools.partial(further, 2 * NZ * step) for step in range(-4, 4)]
    up, dn, hub_rows = lax.switch(dx, firsts, samples, picked)
    up, dn, resid, inverse = lax.switch(dz + 4, seconds, up, dn, samples, hub_rows)
    lo2, lo1, hi1, hi2 = (moved_by(resid, t) for t in (2, 1, -1, -2))
    up, dn = lax.switch(dy + 4, thirds, up, dn)

    blocks = up, dn, resid, lo2, lo1, hi1, hi2
    own, w, v = tiles_of(start % 2, *blocks, hub_rows, inverse)
    diag = jnp.arange(rows)[:, None] == jnp.arange(rows)[None, :]
    own_stat = jnp.where(diag, 0.0, to_stat(own, factor))

    def swapped(which, w, v):
        moves = [j - which for j in range(3)]
        a = [moved_by(w[j], -t) for j, t in enumerate(moves)]
        b = [moved_by(v[j], t) for j, t in enumerate(moves)]
        return jnp.stack(a), jnp.stack(b)

    a, b = lax.switch(back, [functools.partial(swapped, which) for which in range(2)], w, v)
    return (own_stat, to_stat(a, factor), to_stat(b, factor))


def solution(mesh):
    split = Mesh(mesh.devices.reshape(NX, NY, NZ, 2), BLK)
    placed = (P(BLK, None), P(), P())
    return jax.shard_map(
        shards,
        mesh=split,
        in_specs=placed,
        out_specs=(P(BLK, None), P(None, BLK, None), P(None, BLK, None)),
        check_vma=False,
    )
```

```python
import functools
import math

import jax
import jax.numpy as jnp
from jax import lax
from jax.experimental import pallas as pl
from jax.experimental.pallas import tpu as pltpu
from jax.sharding import Mesh
from jax.sharding import PartitionSpec as P

BLK = ("blk_0", "blk_1", "blk_2", "blk_3")
NX, NY, NZ = 4, 8, 8
NDEV = 2 * NX * NY * NZ


def split_up(array, dim, peers):
    before, after = (array.shape[:dim], array.shape[dim + 1 :])
    return jnp.moveaxis(array.reshape(*before, peers, -1, *after), dim, 0)


def sent_and_summed(array, axis, dim):
    tiles = split_up(array, dim, lax.axis_size(axis))
    arrived = lax.all_to_all(tiles, axis, split_axis=0, concat_axis=0, tiled=True)
    return arrived.sum(axis=0)


def sent_to_all(array, axis):
    copies = jnp.broadcast_to(array, (lax.axis_size(axis), *array.shape))
    return lax.all_to_all(copies, axis, split_axis=0, concat_axis=0, tiled=True)


def nested_sum(array, near, far):
    part = sent_and_summed(array, near, 1)
    part = sent_to_all(part, far).sum(axis=0)
    slices = sent_to_all(part, near)
    return jnp.moveaxis(slices, 0, 1).reshape(array.shape)


def moved_by(block, blocks):
    route = [((i - blocks) % NDEV, i) for i in range(NDEV)]
    return lax.ppermute(block, BLK, route) if blocks % NDEV else block


def signed_digit(value, base):
    digit = lax.rem(value + base // 2, base) - base // 2
    return digit, (value - digit) // base


def resid_of(block, hub_rows, inverse):
    exact = lax.Precision.HIGHEST
    proj = lax.dot_general(
        block, hub_rows, (((1,), (1,)), ((), ())), preferred_element_type=jnp.float32
    )
    half = jnp.dot(proj, inverse.T, precision=exact)
    coef = jnp.dot(half, inverse, precision=exact)
    fitted = jnp.dot(coef, hub_rows.astype(jnp.float32), precision=exact)
    return (block.astype(jnp.float32) - fitted).astype(jnp.bfloat16)


def outer_dots(rows, columns):
    return lax.dot_general(
        rows, columns, (((1,), (1,)), ((), ())), preferred_element_type=jnp.float32
    )


def tiles_kernel(odd_ref, up_ref, dn_ref, own_ref, lo2, lo1, hi1, hi2, hub_ref, inv_ref, *outs):
    own_out, w_ref, v_ref, up_res, dn_res = outs
    odd = odd_ref[0] == 1
    exact = lax.Precision.HIGHEST
    hub, inverse = hub_ref[...], inv_ref[...]

    def residual(src, dst):
        block = src[...]
        proj = outer_dots(block, hub)
        half = lax.dot_general(
            proj, inverse, (((1,), (1,)), ((), ())),
            precision=exact, preferred_element_type=jnp.float32,
        )
        rest = jnp.dot(half, inverse, precision=exact, preferred_element_type=jnp.float32)
        pieces = []
        for _ in range(3):
            pieces.append(rest.astype(jnp.bfloat16))
            rest = rest - pieces[-1].astype(jnp.float32)
        for c in range(0, hub.shape[1], 512):
            columns = pl.ds(c, 512)
            part = hub_ref[:, columns]
            fitted = sum(
                jnp.dot(piece, part, preferred_element_type=jnp.float32) for piece in pieces[::-1]
            )
            dst[:, columns] = (src[:, columns].astype(jnp.float32) - fitted).astype(jnp.bfloat16)

    residual(up_ref, up_res)
    residual(dn_ref, dn_res)

    def scale(ref):
        wide = ref[...].astype(jnp.float32)
        return 1.0 / jnp.sqrt(jnp.maximum(jnp.sum(wide * wide, axis=1, keepdims=True), 1.0))

    def turned(column):
        return jnp.transpose(jnp.broadcast_to(column, (column.shape[0], 128)))[:1, :]

    refs = {0: own_ref, 1: hi1, 2: hi2, -1: lo1, -2: lo2}
    scales = {t: scale(ref) for t, ref in refs.items()}
    own = outer_dots(own_ref[...], own_ref[...]) * scales[0] * turned(scales[0])
    own_out[...] = own.astype(jnp.bfloat16)
    up_row, dn_row = turned(scale(up_res)), turned(scale(dn_res))
    for j in range(3):
        def chosen(sign):
            here, there = sign * (j - 1), sign * j
            block = jnp.where(odd, refs[here][...], refs[there][...])
            return block, jnp.where(odd, scales[here], scales[there])

        block, rows = chosen(-1)
        w_ref[j] = (outer_dots(block, dn_res[...]) * rows * dn_row).astype(jnp.bfloat16)
        block, rows = chosen(1)
        v_ref[j] = (outer_dots(block, up_res[...]) * up_row * rows).astype(jnp.bfloat16)


def tiles_of(odd, *arrays):
    rows, dtype = arrays[0].shape[0], arrays[0].dtype
    vmem = pl.BlockSpec(memory_space=pltpu.VMEM)
    return pl.pallas_call(
        tiles_kernel,
        out_shape=[
            jax.ShapeDtypeStruct((rows, rows), dtype),
            jax.ShapeDtypeStruct((3, rows, rows), dtype),
            jax.ShapeDtypeStruct((3, rows, rows), dtype),
        ],
        in_specs=[pl.BlockSpec(memory_space=pltpu.SMEM)] + [vmem] * len(arrays),
        out_specs=[vmem] * 3,
        scratch_shapes=[pltpu.VMEM(arrays[0].shape, dtype)] * 2,
        compiler_params=pltpu.CompilerParams(vmem_limit_bytes=48 * 1024 * 1024),
        cost_estimate=pl.CostEstimate(
            flops=14 * rows * rows * arrays[0].shape[1],
            bytes_accessed=8 * arrays[0].size,
            transcendentals=0,
        ),
        name="tiles",
    )(odd, *arrays)


def to_stat(rounded, factor):
    values = lax.optimization_barrier(rounded).astype(jnp.float32)
    return factor * (0.5 * (jnp.log1p(values) - jnp.log1p(-values)))


def shards(samples, hubs, start):
    rows = samples.shape[0]
    width = samples.shape[1]
    factor = math.sqrt(width - hubs.shape[0] - 3)
    mine = lax.axis_index(BLK)
    owner = hubs // rows
    within = hubs % rows
    picker = jnp.logical_and(
        (owner == mine)[:, None], within[:, None] == jnp.arange(rows, dtype=jnp.int32)[None, :]
    ).astype(jnp.bfloat16)
    picked = jnp.dot(picker, samples, preferred_element_type=jnp.float32).astype(jnp.bfloat16)

    chips = (start[0] + 1) // 2
    back = start[0] % 2
    dz, rest = signed_digit(chips, NZ)
    dy, dx = signed_digit(rest, NY)

    hub_rows = nested_sum(picked, ("blk_2", "blk_3"), ("blk_0", "blk_1"))

    def first(step, samples, hub_rows):
        stride = 2 * NZ * NY * step
        up, dn = moved_by(samples, stride), moved_by(samples, -stride)
        wide = hub_rows.astype(jnp.float32)
        gram = jnp.dot(wide, wide.T, precision=lax.Precision.HIGHEST)
        lower = jnp.linalg.cholesky(gram)
        eye = jnp.eye(gram.shape[0], dtype=jnp.float32)
        inverse = jax.scipy.linalg.solve_triangular(lower, eye, lower=True)
        return up, dn, resid_of(samples, hub_rows, inverse), inverse

    def further(stride, up, dn):
        return moved_by(up, stride), moved_by(dn, -stride)

    firsts = [functools.partial(first, step) for step in range(3)]
    seconds = [functools.partial(further, 2 * NZ * step) for step in range(-4, 4)]
    thirds = [functools.partial(further, 2 * step) for step in range(-4, 4)]
    up, dn, resid, inverse = lax.switch(dx, firsts, samples, hub_rows)
    lo2, lo1, hi1, hi2 = (moved_by(resid, t) for t in (2, 1, -1, -2))
    up, dn = lax.switch(dy + 4, seconds, up, dn)
    up, dn = lax.switch(dz + 4, thirds, up, dn)
    blocks = up, dn, resid, lo2, lo1, hi1, hi2
    own, w, v = tiles_of(start % 2, *blocks, hub_rows, inverse)
    diag = jnp.arange(rows)[:, None] == jnp.arange(rows)[None, :]
    own_stat = jnp.where(diag, 0.0, to_stat(own, factor))

    def swapped(which, w, v):
        moves = [j - which for j in range(3)]
        a = [moved_by(w[j], -t) for j, t in enumerate(moves)]
        b = [moved_by(v[j], t) for j, t in enumerate(moves)]
        return jnp.stack(a), jnp.stack(b)

    a, b = lax.switch(back, [functools.partial(swapped, which) for which in range(2)], w, v)
    return (own_stat, to_stat(a, factor), to_stat(b, factor))


def solution(mesh):
    split = Mesh(mesh.devices.reshape(NX, NY, NZ, 2), BLK)
    placed = (P(BLK, None), P(), P())
    return jax.shard_map(
        shards,
        mesh=split,
        in_specs=placed,
        out_specs=(P(BLK, None), P(None, BLK, None), P(None, BLK, None)),
        check_vma=False,
    )
```

```python
import functools
import math

import jax
import jax.numpy as jnp
from jax import lax
from jax.experimental import pallas as pl
from jax.experimental.pallas import tpu as pltpu
from jax.sharding import Mesh
from jax.sharding import PartitionSpec as P

BLK = ("blk_0", "blk_1", "blk_2", "blk_3")
NX, NY, NZ = 4, 8, 8
NDEV = 2 * NX * NY * NZ


def split_up(array, dim, peers):
    before, after = (array.shape[:dim], array.shape[dim + 1 :])
    return jnp.moveaxis(array.reshape(*before, peers, -1, *after), dim, 0)


def sent_and_summed(array, axis, dim):
    tiles = split_up(array, dim, lax.axis_size(axis))
    arrived = lax.all_to_all(tiles, axis, split_axis=0, concat_axis=0, tiled=True)
    return arrived.sum(axis=0)


def sent_to_all(array, axis):
    copies = jnp.broadcast_to(array, (lax.axis_size(axis), *array.shape))
    return lax.all_to_all(copies, axis, split_axis=0, concat_axis=0, tiled=True)


def nested_sum(array, near, far):
    part = sent_and_summed(array, near, 0)
    part = sent_to_all(part, far).sum(axis=0)
    return sent_to_all(part, near).reshape(array.shape)


def moved_by(block, blocks):
    route = [((i - blocks) % NDEV, i) for i in range(NDEV)]
    return lax.ppermute(block, BLK, route) if blocks % NDEV else block


def signed_digit(value, base):
    digit = lax.rem(value + base // 2, base) - base // 2
    return digit, (value - digit) // base


def resid_of(block, hub_rows, inverse):
    exact = lax.Precision.HIGHEST
    proj = lax.dot_general(
        block, hub_rows, (((1,), (1,)), ((), ())), preferred_element_type=jnp.float32
    )
    half = jnp.dot(proj, inverse.T, precision=exact)
    coef = jnp.dot(half, inverse, precision=exact)
    fitted = jnp.dot(coef, hub_rows.astype(jnp.float32), precision=exact)
    return (block.astype(jnp.float32) - fitted).astype(jnp.bfloat16)


def outer_dots(rows, columns):
    return lax.dot_general(
        rows, columns, (((1,), (1,)), ((), ())), preferred_element_type=jnp.float32
    )


def tiles_kernel(odd_ref, up_ref, dn_ref, own_ref, lo2, lo1, hi1, hi2, hub_ref, inv_ref, *outs):
    own_out, w_ref, v_ref, up_res, dn_res = outs
    odd = odd_ref[0] == 1
    exact = lax.Precision.HIGHEST
    hub, inverse = hub_ref[...], inv_ref[...]

    def residual(src, dst):
        block = src[...]
        proj = outer_dots(block, hub)
        half = lax.dot_general(
            proj, inverse, (((1,), (1,)), ((), ())),
            precision=exact, preferred_element_type=jnp.float32,
        )
        rest = jnp.dot(half, inverse, precision=exact, preferred_element_type=jnp.float32)
        pieces = []
        for _ in range(3):
            pieces.append(rest.astype(jnp.bfloat16))
            rest = rest - pieces[-1].astype(jnp.float32)
        for c in range(0, hub.shape[1], 512):
            columns = pl.ds(c, 512)
            part = hub_ref[:, columns]
            fitted = sum(
                jnp.dot(piece, part, preferred_element_type=jnp.float32) for piece in pieces[::-1]
            )
            dst[:, columns] = (src[:, columns].astype(jnp.float32) - fitted).astype(jnp.bfloat16)

    residual(up_ref, up_res)
    residual(dn_ref, dn_res)

    def scale(ref):
        wide = ref[...].astype(jnp.float32)
        return 1.0 / jnp.sqrt(jnp.maximum(jnp.sum(wide * wide, axis=1, keepdims=True), 1.0))

    def turned(column):
        return jnp.transpose(jnp.broadcast_to(column, (column.shape[0], 128)))[:1, :]

    refs = {0: own_ref, 1: hi1, 2: hi2, -1: lo1, -2: lo2}
    scales = {t: scale(ref) for t, ref in refs.items()}
    own = outer_dots(own_ref[...], own_ref[...]) * scales[0] * turned(scales[0])
    own_out[...] = own.astype(jnp.bfloat16)
    up_row, dn_row = turned(scale(up_res)), turned(scale(dn_res))
    for j in range(3):
        def chosen(sign):
            here, there = sign * (j - 1), sign * j
            block = jnp.where(odd, refs[here][...], refs[there][...])
            return block, jnp.where(odd, scales[here], scales[there])

        block, rows = chosen(-1)
        w_ref[j] = (outer_dots(block, dn_res[...]) * rows * dn_row).astype(jnp.bfloat16)
        block, rows = chosen(1)
        v_ref[j] = (outer_dots(block, up_res[...]) * up_row * rows).astype(jnp.bfloat16)


def tiles_of(odd, *arrays):
    rows, dtype = arrays[0].shape[0], arrays[0].dtype
    vmem = pl.BlockSpec(memory_space=pltpu.VMEM)
    return pl.pallas_call(
        tiles_kernel,
        out_shape=[
            jax.ShapeDtypeStruct((rows, rows), dtype),
            jax.ShapeDtypeStruct((3, rows, rows), dtype),
            jax.ShapeDtypeStruct((3, rows, rows), dtype),
        ],
        in_specs=[pl.BlockSpec(memory_space=pltpu.SMEM)] + [vmem] * len(arrays),
        out_specs=[vmem] * 3,
        scratch_shapes=[pltpu.VMEM(arrays[0].shape, dtype)] * 2,
        compiler_params=pltpu.CompilerParams(vmem_limit_bytes=48 * 1024 * 1024),
        cost_estimate=pl.CostEstimate(
            flops=14 * rows * rows * arrays[0].shape[1],
            bytes_accessed=8 * arrays[0].size,
            transcendentals=0,
        ),
        name="tiles",
    )(odd, *arrays)


def to_stat(rounded, factor):
    values = lax.optimization_barrier(rounded).astype(jnp.float32)
    return factor * (0.5 * (jnp.log1p(values) - jnp.log1p(-values)))


def shards(samples, hubs, start):
    rows = samples.shape[0]
    width = samples.shape[1]
    factor = math.sqrt(width - hubs.shape[0] - 3)
    mine = lax.axis_index(BLK)
    owner = hubs // rows
    within = hubs % rows
    picker = jnp.logical_and(
        (owner == mine)[:, None], within[:, None] == jnp.arange(rows, dtype=jnp.int32)[None, :]
    ).astype(jnp.bfloat16)
    picked = jnp.dot(picker, samples, preferred_element_type=jnp.float32).astype(jnp.bfloat16)

    chips = (start[0] + 1) // 2
    back = start[0] % 2
    dz, rest = signed_digit(chips, NZ)
    dy, dx = signed_digit(rest, NY)

    hub_rows = nested_sum(picked, ("blk_0", "blk_1"), ("blk_2", "blk_3"))

    def first(step, samples, hub_rows):
        stride = 2 * NZ * NY * step
        up, dn = moved_by(samples, stride), moved_by(samples, -stride)
        wide = hub_rows.astype(jnp.float32)
        gram = jnp.dot(wide, wide.T, precision=lax.Precision.HIGHEST)
        lower = jnp.linalg.cholesky(gram)
        eye = jnp.eye(gram.shape[0], dtype=jnp.float32)
        inverse = jax.scipy.linalg.solve_triangular(lower, eye, lower=True)
        return up, dn, resid_of(samples, hub_rows, inverse), inverse

    def further(stride, up, dn):
        return moved_by(up, stride), moved_by(dn, -stride)

    firsts = [functools.partial(first, step) for step in range(3)]
    seconds = [functools.partial(further, 2 * NZ * step) for step in range(-4, 4)]
    thirds = [functools.partial(further, 2 * step) for step in range(-4, 4)]
    up, dn, resid, inverse = lax.switch(dx, firsts, samples, hub_rows)
    lo2, lo1, hi1, hi2 = (moved_by(resid, t) for t in (2, 1, -1, -2))
    up, dn = lax.switch(dy + 4, seconds, up, dn)
    up, dn = lax.switch(dz + 4, thirds, up, dn)
    blocks = up, dn, resid, lo2, lo1, hi1, hi2
    own, w, v = tiles_of(start % 2, *blocks, hub_rows, inverse)
    diag = jnp.arange(rows)[:, None] == jnp.arange(rows)[None, :]
    own_stat = jnp.where(diag, 0.0, to_stat(own, factor))

    def swapped_even(w, v):
        a = [moved_by(w[t], -t) for t in range(3)]
        b = [moved_by(v[t], t) for t in range(3)]
        return jnp.stack(a), jnp.stack(b)

    def swapped_odd(w, v):
        later = moved_by(jnp.stack([w[0], v[2]]), 1)
        sooner = moved_by(jnp.stack([w[2], v[0]]), -1)
        return jnp.stack([later[0], w[1], sooner[0]]), jnp.stack([sooner[1], v[1], later[1]])

    a, b = lax.switch(back, [swapped_even, swapped_odd], w, v)
    return (own_stat, to_stat(a, factor), to_stat(b, factor))


def solution(mesh):
    split = Mesh(mesh.devices.reshape(NX, NY, NZ, 2), BLK)
    placed = (P(BLK, None), P(), P())
    return jax.shard_map(
        shards,
        mesh=split,
        in_specs=placed,
        out_specs=(P(BLK, None), P(None, BLK, None), P(None, BLK, None)),
        check_vma=False,
    )
```
